32 devices in a mesh: tp: 8 (over y, x, core), dp: 4 (over z).
Axes of the slice: x: 2, y: 2, z: 4, core: 2. Of those that a mesh axis runs over, the one named last changes fastest.
Arguments:
- grad_out: bfloat16 [512, 16384], P('dp', 'tp'), may hold values from -6 to 6
- hidden_sum: bfloat16 [512, 16384], P('dp', 'tp'), may hold values from -100 to 100
- norm_gain: float32 [16384], P('tp'), may hold values from 0.5 to 1.5
- out_weight: bfloat16 [2048, 16384], P(None, 'tp'), may hold values from -0.046875 to 0.046875
Outputs:
- resid_grad: bfloat16 [512, 16384], P('dp', 'tp')
- attn_grad: bfloat16 [512, 2048], P('dp', 'tp')
- gain_grad: float32 [16384], P('tp')
The draws below stay inside these ranges and needn't reach their ends.
All inputs are finite; a program needn't handle non-finite values.
Results may differ from the reference program's by a relative error of at most 0.0049.
Values sent between devices are 32-bit elements; how exact they have to be, the bound alone decides.
A program may use at most 64 MiB of HBM per device.

```python
import math
import jax
import jax.numpy as jnp
from jax import lax

D = 16384
TOKENS = 512
D_IN = 2048


def draw_hidden_sum(key, part):
    key_values, key_row, key_col = jax.random.split(jax.random.fold_in(key, 11), 3)
    position = jnp.arange(D, dtype=jnp.float32) / D
    column = jnp.exp(math.log(3.0) * position + math.log(10.0) * jax.random.uniform(key_col, (D,), jnp.float32))
    column = column / jnp.sqrt(jnp.mean(column * column))
    values = jnp.clip(jax.random.normal(key_values, (TOKENS, D), jnp.float32), -4.0, 4.0)
    row_scale = jnp.exp(jax.random.uniform(key_row, (TOKENS, 1), jnp.float32, minval=math.log(0.3), maxval=math.log(3.0)))
    return jnp.clip(values * row_scale * column, -100.0, 100.0).astype(jnp.bfloat16)


def steps_of(own_key, dims, cuts, low, largest):
    level = 1.0
    for dim, blocks in cuts:
        steps = jax.random.uniform(jax.random.fold_in(jax.random.fold_in(own_key, 6), dim), (blocks,), jnp.float32, low / len(cuts), largest / len(cuts))
        level = level * jnp.repeat(jnp.exp(steps), dims[dim] // blocks).reshape((-1,) + (1,) * (len(dims) - 1 - dim))
    return level


def normal_values(own_key, dims, deviation, most, cuts=(), kind=jnp.bfloat16):
    array = deviation * jax.random.normal(own_key, dims, jnp.float32)
    if cuts:
        array = array * steps_of(own_key, dims, cuts, -0.22, 0.18)
    return jnp.clip(array, -most, most).astype(kind)


def setup_inputs(seed: int = 0) -> dict:
    seeds = jax.random.split(jax.random.key(seed), 5)
    grad_out = normal_values(seeds[0], (TOKENS, D), 1.0, 6.0, ((0, 4), (1, 8)))
    hidden_sum = draw_hidden_sum(jax.random.fold_in(seeds[4], 71), 0)
    norm_gain = jnp.clip(0.5 + 1.0 * jax.random.uniform(seeds[2], (D,), jnp.float32) ** steps_of(seeds[2], (D,), ((0, 8),), -0.2, 0.2), 0.5, 1.5)
    out_weight = normal_values(seeds[3], (D_IN, D), D ** -0.5, 0.046875, ((1, 8),))
    return dict(grad_out=grad_out, hidden_sum=hidden_sum, norm_gain=norm_gain, out_weight=out_weight)


epsilon = 1e-05

def backward_rows(upstream_b, stream_b, norm_gain, out_weight):
    upstream = upstream_b.astype(jnp.float32)
    stream = stream_b.astype(jnp.float32)
    squares = lax.optimization_barrier(jnp.sum(stream * stream, axis=1))
    inverse = lax.rsqrt(squares / D + epsilon)
    dotted = lax.optimization_barrier(jnp.sum(norm_gain * upstream * stream, axis=1))
    factor = inverse * inverse * dotted / D
    resid_full = inverse[:, None] * (norm_gain * upstream - stream * factor[:, None])
    resid_grad = resid_full.astype(jnp.bfloat16)
    attn_grad = jnp.dot(resid_grad, out_weight.T, preferred_element_type=jnp.float32).astype(jnp.bfloat16)
    gain_part = lax.optimization_barrier(jnp.sum(upstream * stream * inverse[:, None], axis=0))
    return (resid_grad, attn_grad, gain_part)

def reference(grad_out, hidden_sum, norm_gain, out_weight):
    span_rows = math.gcd(TOKENS, 512)
    number = TOKENS // span_rows

    def advance(carry, pieces):
        resid_grad, attn_grad, gain_part = backward_rows(pieces[0], pieces[1], norm_gain, out_weight)
        return (carry + gain_part, (resid_grad, attn_grad))
    gain_grad, outputs = lax.scan(advance, jnp.zeros((D,), jnp.float32), (grad_out.reshape(number, span_rows, D), hidden_sum.reshape(number, span_rows, D)))
    return (outputs[0].reshape(TOKENS, D), outputs[1].reshape(TOKENS, D_IN), gain_grad)
```

```python
import functools

import jax
import jax.numpy as jnp
from jax import lax
from jax.experimental import pallas as pl
from jax.experimental.pallas import tpu as pltpu
from jax.sharding import PartitionSpec as P

EPSILON = 1e-05
MESH = pl.DeviceIdType.MESH
LANES = 128
CHUNKS = 1


def flipped(index, mask):
    result, bit = index, 1
    while bit <= mask:
        if mask & bit:
            result = result + bit * (1 - 2 * lax.rem(lax.div(index, bit), 2))
        bit *= 2
    return result


def kernel(
    tp, dp, features,
    grad_hbm, hidden_hbm, gain_hbm, weight_hbm,
    resid, attn, gain_out,
    grad, both, gain_ref, weight, stats, pair_out, pair_in, pair_own, chip_out, chip_in, relay_in, sums,
    load_sem, weight_sem,
    stat_send, stat_recv, pair_send, pair_recv, chip_send, chip_recv,
    relay_send, relay_recv, sum_send, sum_recv, ready,
):
    me = lax.axis_index("tp")
    z = lax.axis_index("dp")
    rows, width = grad.shape
    block = attn.shape[1]
    hidden = both.at[pl.ds(rows, rows), :]
    steps = width // LANES

    load_grad = pltpu.make_async_copy(grad_hbm, grad, load_sem.at[0])
    load_hidden = pltpu.make_async_copy(hidden_hbm, hidden, load_sem.at[1])
    load_gain = pltpu.make_async_copy(gain_hbm, gain_ref, load_sem.at[2])
    load_hidden.start()
    load_grad.start()
    load_gain.start()

    barrier = pltpu.get_barrier_semaphore()
    for mask in range(1, tp):
        pl.semaphore_signal(
            barrier, inc=1, device_id={"tp": flipped(me, mask)}, device_id_type=MESH
        )
    for step in range(1, dp):

        @pl.when(z + step < dp)
        def _():
            pl.semaphore_signal(
                barrier, inc=1, device_id={"dp": z + step}, device_id_type=MESH
            )


    order = sorted(range(0, tp, 2), key=lambda mask: (-bin(mask).count("1"), mask))

    def weight_rows(mask):
        return pl.ds(pl.multiple_of(flipped(me, mask) * block, block), block)

    weight_loads = {}
    for chip in order:
        for mask in (chip ^ 1, chip):
            at = weight_rows(mask)
            weight_loads[mask] = pltpu.make_async_copy(
                weight_hbm.at[at, :], weight.at[mask], weight_sem.at[mask]
            )
            weight_loads[mask].start()

    load_gain.wait()
    load_hidden.wait()
    load_grad.wait()
    squares = jnp.zeros((rows, LANES), jnp.float32)
    dotted = jnp.zeros((rows, LANES), jnp.float32)
    for k in range(steps):
        at = slice(k * LANES, (k + 1) * LANES)
        h = hidden[:, at].astype(jnp.float32)
        g = grad[:, at].astype(jnp.float32)
        squares += h * h
        dotted += gain_ref[:, at] * g * h
    local_factor = jnp.sum(dotted, axis=1, keepdims=True) / (
        jnp.sum(squares, axis=1, keepdims=True) + width * EPSILON
    )
    stats[0, 0:1, :] = jnp.sum(squares.T, axis=0, keepdims=True)
    stats[0, 1:2, :] = jnp.sum(dotted.T, axis=0, keepdims=True)

    pl.semaphore_wait(barrier, tp - 1 + z)
    stat_copies = []
    for mask in sorted(range(1, tp), key=lambda mask: (-bin(mask).count("1"), mask)):
        copy = pltpu.make_async_remote_copy(
            src_ref=stats.at[0],
            dst_ref=stats.at[mask],
            send_sem=stat_send.at[mask],
            recv_sem=stat_recv.at[mask],
            device_id={"tp": flipped(me, mask)},
            device_id_type=MESH,
        )
        copy.start()
        stat_copies.append(copy)
    for step in range(1, dp):

        @pl.when(z >= step)
        def _():
            pl.semaphore_signal(
                ready, inc=1, device_id={"dp": z - step}, device_id_type=MESH
            )

    for k in range(steps):
        at = slice(k * LANES, (k + 1) * LANES)
        h = hidden[:, at].astype(jnp.float32)
        g = grad[:, at].astype(jnp.float32)
        both[0:rows, at] = (gain_ref[:, at] * g - h * local_factor).astype(jnp.bfloat16)

    def products(mask, target):
        out = lax.dot_general(
            both[...],
            weight[mask],
            (((1,), (1,)), ((), ())),
            preferred_element_type=jnp.float32,
        )
        target[0] = out[0:rows] + local_factor * out[rows:]
        target[1] = out[rows:]

    pair_copies = []

    def pair_step(slot):
        chip = order[slot]
        weight_loads[chip ^ 1].wait()
        weight_loads[chip].wait()
        products(chip ^ 1, pair_out.at[slot])
        copy = pltpu.make_async_remote_copy(
            src_ref=pair_out.at[slot],
            dst_ref=pair_in.at[slot],
            send_sem=pair_send.at[slot],
            recv_sem=pair_recv.at[slot],
            device_id={"tp": flipped(me, 1)},
            device_id_type=MESH,
        )
        products(chip, pair_own.at[slot])
        copy.start()
        pair_copies.append(copy)

    last = len(order) - 1
    for slot in range(last):
        pair_step(slot)

    for copy in stat_copies:
        copy.wait_recv()
    total = stats[0]
    for mask in range(1, tp):
        total = total + stats[mask]
    inverse_row = lax.rsqrt(total[0:1, :] / features + EPSILON)
    factor_row = inverse_row * inverse_row * total[1:2, :] / features
    inverse = jnp.broadcast_to(inverse_row, (LANES, rows)).T
    factor = jnp.broadcast_to(factor_row, (LANES, rows)).T

    pieces = block // LANES
    relayed = len(order) == 4 and pieces % 2 == 0
    chunk = rows // CHUNKS

    def chip_piece(slot, piece):
        at = slice(piece * LANES, (piece + 1) * LANES)
        gained = pair_own[slot, 0, :, at] + pair_in[slot, 0, :, at]
        plain = pair_own[slot, 1, :, at] + pair_in[slot, 1, :, at]
        chip_out[slot, piece] = inverse * (gained - factor * plain)

    def send(slot, piece, part):
        at = pl.ds(part * chunk, chunk)
        copy = pltpu.make_async_remote_copy(
            src_ref=chip_out.at[slot, piece, at],
            dst_ref=chip_in.at[slot, piece, at],
            send_sem=chip_send.at[slot, piece, part],
            recv_sem=chip_recv.at[slot, piece, part],
            device_id={"tp": flipped(me, order[slot])},
            device_id_type=MESH,
        )
        copy.start()
        return copy

    def pass_on(piece, part):
        at = pl.ds(part * chunk, chunk)
        copy = pltpu.make_async_remote_copy(
            src_ref=chip_out.at[0, piece, at],
            dst_ref=relay_in.at[piece, at],
            send_sem=relay_send.at[piece, part],
            recv_sem=relay_recv.at[piece, part],
            device_id={"tp": flipped(me, order[1 + piece % 2])},
            device_id_type=MESH,
        )
        copy.start()
        return copy

    chip_copies, relay_copies = [], []
    pair_copies[0].wait_recv()
    for piece in range(pieces):
        chip_piece(0, piece)
        for part in range(CHUNKS):
            if relayed:
                relay_copies.append((piece, part, pass_on(piece, part)))
            else:
                chip_copies.append(send(0, piece, part))
    for slot in range(1, last):
        pair_copies[slot].wait_recv()
        for piece in range(pieces):
            chip_piece(slot, piece)
            if not relayed or piece % 2 == slot - 1:
                for part in range(CHUNKS):
                    chip_copies.append(send(slot, piece, part))

    for k in range(steps):
        at = slice(k * LANES, (k + 1) * LANES)
        h = hidden[:, at].astype(jnp.float32)
        g = grad[:, at].astype(jnp.float32)
        sums[0, :, at] = jnp.sum(g * h * inverse, axis=0, keepdims=True)
    sum_copies = []
    for step in range(dp - 1, 0, -1):
        copy = pltpu.make_async_remote_copy(
            src_ref=sums.at[0],
            dst_ref=sums.at[step],
            send_sem=sum_send.at[step],
            recv_sem=sum_recv.at[step],
            device_id={"dp": lax.rem(z + step, dp)},
            device_id_type=MESH,
        )
        pl.when(z + step >= dp)(copy.start)
        sum_copies.append(copy)

    pair_step(last)

    for k in range(steps):
        at = slice(k * LANES, (k + 1) * LANES)
        h = hidden[:, at].astype(jnp.float32)
        g = grad[:, at].astype(jnp.float32)
        value = inverse * (gain_ref[:, at] * g - h * factor)
        resid[:, at] = value.astype(jnp.bfloat16)

    @pl.when(z < dp - 1)
    def _():
        pl.semaphore_wait(ready, dp - 1 - z)

    for step, copy in zip(range(dp - 1, 0, -1), sum_copies):
        pl.when(z + step < dp)(copy.start)

    for part in range(CHUNKS):
        for piece, own_part, copy in relay_copies:
            if own_part == part:
                slot = 2 - piece % 2
                at = slice(part * chunk, (part + 1) * chunk)
                copy.wait_recv()
                chip_out[slot, piece, at] = chip_out[slot, piece, at] + relay_in[piece, at]
                chip_copies.append(send(slot, piece, part))

    pair_copies[last].wait_recv()
    for piece in range(pieces):
        chip_piece(last, piece)

    for copy in sum_copies:
        copy.wait_recv()
    gain_total = sums[0]
    for step in range(1, dp):
        gain_total = gain_total + sums[step]
    gain_out[...] = gain_total

    for copy in chip_copies:
        copy.wait_recv()
    for piece in range(pieces):
        result = chip_out[last, piece]
        for slot in range(1 if relayed else 0, last):
            result = result + chip_in[slot, piece]
        attn[:, piece * LANES : (piece + 1) * LANES] = result

    for copy in stat_copies + pair_copies + chip_copies + sum_copies:
        copy.wait_send()
    for _, _, copy in relay_copies:
        copy.wait_send()


def write_results(resid, attn, gain, resid_out, attn_out, gain_out):
    resid_out[...] = resid[...]
    attn_out[...] = attn[...].astype(jnp.bfloat16)
    gain_out[...] = gain[...]


def on_device(tp, dp, features, grad_out, hidden_sum, norm_gain, out_weight):
    rows, width = grad_out.shape
    block = out_weight.shape[0] // tp
    half = tp // 2
    pieces = block // LANES
    anywhere = pl.BlockSpec(memory_space=pltpu.HBM)
    vmem = pl.BlockSpec(memory_space=pltpu.VMEM)
    dma = pltpu.SemaphoreType.DMA
    resid, attn, gain = pl.pallas_call(
        functools.partial(kernel, tp, dp, features),
        out_shape=(
            jax.ShapeDtypeStruct((rows, width), jnp.bfloat16),
            jax.ShapeDtypeStruct((rows, block), jnp.float32),
            jax.ShapeDtypeStruct((1, width), jnp.float32),
        ),
        in_specs=[anywhere, anywhere, anywhere, anywhere],
        out_specs=(vmem, vmem, vmem),
        scratch_shapes=[
            pltpu.VMEM((rows, width), jnp.bfloat16),
            pltpu.VMEM((2 * rows, width), jnp.bfloat16),
            pltpu.VMEM((1, width), jnp.float32),
            pltpu.VMEM((tp, block, width), jnp.bfloat16),
            pltpu.VMEM((tp, 2, rows), jnp.float32),
            pltpu.VMEM((half, 2, rows, block), jnp.float32),
            pltpu.VMEM((half, 2, rows, block), jnp.float32),
            pltpu.VMEM((half, 2, rows, block), jnp.float32),
            pltpu.VMEM((half, pieces, rows, LANES), jnp.float32),
            pltpu.VMEM((half, pieces, rows, LANES), jnp.float32),
            pltpu.VMEM((pieces, rows, LANES), jnp.float32),
            pltpu.VMEM((dp, 1, width), jnp.float32),
            dma((3,)),
            dma((tp,)),
            dma((tp,)),
            dma((tp,)),
            dma((half,)),
            dma((half,)),
            dma((half, pieces, CHUNKS)),
            dma((half, pieces, CHUNKS)),
            dma((pieces, CHUNKS)),
            dma((pieces, CHUNKS)),
            dma((dp,)),
            dma((dp,)),
            pltpu.SemaphoreType.REGULAR,
        ],
        compiler_params=pltpu.CompilerParams(
            collective_id=0, has_side_effects=True, vmem_limit_bytes=52 * 2**20
        ),
        name="backward",
    )(
        pltpu.with_memory_space_constraint(grad_out, pltpu.HBM),
        pltpu.with_memory_space_constraint(hidden_sum, pltpu.HBM),
        pltpu.with_memory_space_constraint(norm_gain.reshape(1, width), pltpu.HBM),
        pltpu.with_memory_space_constraint(out_weight, pltpu.HBM),
    )
    resid, attn, gain = pl.pallas_call(
        write_results,
        out_shape=(
            jax.ShapeDtypeStruct((rows, width), jnp.bfloat16),
            jax.ShapeDtypeStruct((rows, block), jnp.bfloat16),
            jax.ShapeDtypeStruct((1, width), jnp.float32),
        ),
        in_specs=[vmem, vmem, vmem],
        out_specs=(vmem, vmem, vmem),
        compiler_params=pltpu.CompilerParams(vmem_limit_bytes=4 * 2**20),
        name="write_results",
    )(resid, attn, gain)
    return resid, attn, gain.reshape(width)


def solution(mesh):
    tp, dp = mesh.shape["tp"], mesh.shape["dp"]

    def whole(grad_out, hidden_sum, norm_gain, out_weight):
        features = grad_out.shape[1]
        return jax.shard_map(
            functools.partial(on_device, tp, dp, features),
            mesh=mesh,
            in_specs=(P("dp", "tp"), P("dp", "tp"), P("tp"), P(None, "tp")),
            out_specs=(P("dp", "tp"), P("dp", "tp"), P("tp")),
            check_vma=False,
        )(grad_out, hidden_sum, norm_gain, out_weight)

    return whole
```

```python
import functools

import jax
import jax.numpy as jnp
from jax import lax
from jax.experimental import pallas as pl
from jax.experimental.pallas import tpu as pltpu
from jax.sharding import PartitionSpec as P

EPSILON = 1e-05
MESH = pl.DeviceIdType.MESH
LANES = 128
BANDS = 4


def flipped(index, mask):
    result, bit = index, 1
    while bit <= mask:
        if mask & bit:
            result = result + bit * (1 - 2 * lax.rem(lax.div(index, bit), 2))
        bit *= 2
    return result


def cuts(rows, relayed):
    if not relayed:
        return [(0, rows)]
    half, quarter = rows // 2, rows // 4
    return [(0, half), (half, quarter), (half + quarter, quarter)]


def kernel(
    tp, dp, features,
    grad_hbm, hidden_hbm, gain_hbm, weight_hbm,
    resid, attn, gain_out,
    grad, both, gain_ref, weight, stats, pair_out, pair_in, pair_own, chip_out, chip_in,
    early_out, early_in, relay_in, sums,
    load_sem, weight_sem, send_sem, stat_recv, pair_recv, early_recv, relay_recv, chip_recv,
    sum_recv, ready,
):
    me = lax.axis_index("tp")
    z = lax.axis_index("dp")
    core = lax.rem(me, 2)
    rows, width = grad.shape
    block = attn.shape[1]
    hidden = both.at[pl.ds(rows, rows), :]
    steps = width // LANES
    band = rows // BANDS
    pieces = block // LANES
    order = sorted(range(0, tp, 2), key=lambda mask: (-bin(mask).count("1"), mask))
    last = len(order) - 1
    relayed = len(order) == 4 and pieces % 2 == 0
    parts = cuts(rows, relayed)
    early = parts[0][1]

    def remote(source, target, kind, recv_sem, axis, index):
        return pltpu.make_async_remote_copy(
            src_ref=source,
            dst_ref=target,
            send_sem=send_sem.at[kind],
            recv_sem=recv_sem,
            device_id={axis: index},
            device_id_type=MESH,
        )

    def wait_bytes(ref, sem):
        pltpu.make_async_copy(ref, ref, sem).wait()

    load_gain = pltpu.make_async_copy(gain_hbm, gain_ref, load_sem.at[BANDS])
    for part in range(BANDS):
        at = pl.ds(part * band, band)
        pltpu.make_async_copy(
            hidden_hbm.at[at, :],
            both.at[pl.ds(rows + part * band, band), :],
            load_sem.at[part],
        ).start()
        pltpu.make_async_copy(grad_hbm.at[at, :], grad.at[at, :], load_sem.at[part]).start()
        if part == 0:
            load_gain.start()

    barrier = pltpu.get_barrier_semaphore()
    for mask in range(1, tp):
        pl.semaphore_signal(
            barrier, inc=1, device_id={"tp": flipped(me, mask)}, device_id_type=MESH
        )
    for step in range(1, dp):

        @pl.when(z + step < dp)
        def _():
            pl.semaphore_signal(
                barrier, inc=1, device_id={"dp": z + step}, device_id_type=MESH
            )

    weight_loads = []
    for slot, chip in enumerate(order):
        start = pl.multiple_of((flipped(me, chip) - core) * block, 2 * block)
        load = pltpu.make_async_copy(
            weight_hbm.at[pl.ds(start, 2 * block), :], weight.at[slot], weight_sem.at[slot]
        )
        load.start()
        weight_loads.append(load)

    load_gain.wait()
    squares, dotted = [], []
    for part in range(BANDS):
        wait_bytes(grad.at[pl.ds(0, 2 * band), :], load_sem.at[part])
        at_rows = slice(part * band, (part + 1) * band)
        band_squares = jnp.zeros((band, LANES), jnp.float32)
        band_dotted = jnp.zeros((band, LANES), jnp.float32)
        for k in range(steps):
            at = slice(k * LANES, (k + 1) * LANES)
            h = hidden[at_rows, at].astype(jnp.float32)
            g = grad[at_rows, at].astype(jnp.float32)
            band_squares += h * h
            band_dotted += gain_ref[:, at] * g * h
        squares.append(band_squares)
        dotted.append(band_dotted)
    squares = jnp.concatenate(squares, axis=0)
    dotted = jnp.concatenate(dotted, axis=0)
    local_factor = jnp.sum(dotted, axis=1, keepdims=True) / (
        jnp.sum(squares, axis=1, keepdims=True) + width * EPSILON
    )
    stats[0, 0:1, :] = jnp.sum(squares.T, axis=0, keepdims=True)
    stats[0, 1:2, :] = jnp.sum(dotted.T, axis=0, keepdims=True)

    pl.semaphore_wait(barrier, tp - 1 + z)
    for mask in sorted(range(1, tp), key=lambda mask: (-bin(mask).count("1"), mask)):
        remote(
            stats.at[0], stats.at[mask], 0, stat_recv, "tp", flipped(me, mask)
        ).start()
    for step in range(1, dp):

        @pl.when(z >= step)
        def _():
            pl.semaphore_signal(
                ready, inc=1, device_id={"dp": z - step}, device_id_type=MESH
            )

    for k in range(steps):
        at = slice(k * LANES, (k + 1) * LANES)
        h = hidden[:, at].astype(jnp.float32)
        g = grad[:, at].astype(jnp.float32)
        both[0:rows, at] = (gain_ref[:, at] * g - h * local_factor).astype(jnp.bfloat16)

    def products(slot, which, target):
        out = lax.dot_general(
            both[...],
            weight[slot, pl.ds(pl.multiple_of(which * block, block), block)],
            (((1,), (1,)), ((), ())),
            preferred_element_type=jnp.float32,
        )
        target[0] = out[0:rows] + local_factor * out[rows:]
        target[1] = out[rows:]

    pair_copies = []

    def pair_step(slot):
        weight_loads[slot].wait()
        products(slot, 1 - core, pair_out.at[slot])
        products(slot, core, pair_own.at[slot])
        copy = remote(
            pair_out.at[slot], pair_in.at[slot], 1, pair_recv.at[slot], "tp", flipped(me, 1)
        )
        copy.start()
        pair_copies.append(copy)

    for slot in range(last):
        pair_step(slot)

    def relay(piece, source, target, kind, recv_sem):
        copy = remote(
            source, target, kind, recv_sem, "tp", flipped(me, order[1 + piece % 2])
        )
        copy.start()
        return copy

    early_copies = []
    pair_copies[0].wait_recv()
    if relayed:
        for piece in range(pieces):
            at = slice(piece * LANES, (piece + 1) * LANES)
            for plane in range(2):
                early_out[piece, plane] = (
                    pair_own[0, plane, 0:early, at] + pair_in[0, plane, 0:early, at]
                )
            early_copies.append(
                relay(piece, early_out.at[piece], early_in.at[piece], 2, early_recv.at[piece])
            )

    wait_bytes(stats.at[pl.ds(1, tp - 1)], stat_recv)
    total = stats[0]
    for mask in range(1, tp):
        total = total + stats[mask]
    inverse_row = lax.rsqrt(total[0:1, :] / features + EPSILON)
    factor_row = inverse_row * inverse_row * total[1:2, :] / features
    inverse = jnp.broadcast_to(inverse_row, (LANES, rows)).T
    factor = jnp.broadcast_to(factor_row, (LANES, rows)).T

    def chip_piece(slot, piece, low=0, high=rows):
        at = slice(piece * LANES, (piece + 1) * LANES)
        own, got = pair_own.at[slot, :, low:high, at], pair_in.at[slot, :, low:high, at]
        gained = own[0] + got[0]
        plain = own[1] + got[1]
        chip_out[slot, piece, low:high] = inverse[low:high] * (
            gained - factor[low:high] * plain
        )

    def send(slot, piece, part):
        at = pl.ds(*parts[part])
        remote(
            chip_out.at[slot, piece, at],
            chip_in.at[slot, piece, at],
            3,
            chip_recv,
            "tp",
            flipped(me, order[slot]),
        ).start()

    relay_copies = []
    if relayed:
        for part in range(1, len(parts)):
            low, size = parts[part]
            for piece in range(pieces):
                chip_piece(0, piece, low, low + size)
                relay_copies.append(
                    relay(
                        piece,
                        chip_out.at[0, piece, pl.ds(low, size)],
                        relay_in.at[piece, pl.ds(low, size)],
                        4,
                        relay_recv.at[piece, part - 1],
                    )
                )
    else:
        for piece in range(pieces):
            chip_piece(0, piece)
            send(0, piece, 0)
    for slot in range(1, last):
        pair_copies[slot].wait_recv()
        for piece in range(pieces):
            chip_piece(slot, piece)
            if not relayed or piece % 2 == slot - 1:
                for part in range(len(parts)):
                    send(slot, piece, part)

    for k in range(steps):
        at = slice(k * LANES, (k + 1) * LANES)
        h = hidden[:, at].astype(jnp.float32)
        g = grad[:, at].astype(jnp.float32)
        sums[0, :, at] = jnp.sum(g * h * inverse, axis=0, keepdims=True)
    sum_copies = []
    for step in range(dp - 1, 0, -1):
        copy = remote(
            sums.at[0], sums.at[step], 5, sum_recv, "dp", lax.rem(z + step, dp)
        )
        pl.when(z + step >= dp)(copy.start)
        sum_copies.append((step, copy))

    pair_step(last)

    for k in range(steps):
        at = slice(k * LANES, (k + 1) * LANES)
        h = hidden[:, at].astype(jnp.float32)
        g = grad[:, at].astype(jnp.float32)
        value = inverse * (gain_ref[:, at] * g - h * factor)
        resid[:, at] = value.astype(jnp.bfloat16)

    @pl.when(z < dp - 1)
    def _():
        pl.semaphore_wait(ready, dp - 1 - z)

    for step, copy in sum_copies:
        pl.when(z + step < dp)(copy.start)

    if relayed:
        for piece in range(pieces):
            slot = 2 - piece % 2
            early_copies[piece].wait_recv()
            chip_out[slot, piece, 0:early] = chip_out[slot, piece, 0:early] + inverse[
                0:early
            ] * (early_in[piece, 0] - factor[0:early] * early_in[piece, 1])
            send(slot, piece, 0)
        for i, copy in enumerate(relay_copies):
            part, piece = 1 + i // pieces, i % pieces
            slot = 2 - piece % 2
            low, size = parts[part]
            at = slice(low, low + size)
            copy.wait_recv()
            chip_out[slot, piece, at] = chip_out[slot, piece, at] + relay_in[piece, at]
            send(slot, piece, part)

    pair_copies[last].wait_recv()
    for piece in range(pieces):
        chip_piece(last, piece)

    wait_bytes(sums.at[pl.ds(1, dp - 1)], sum_recv)
    gain_total = sums[0]
    for step in range(1, dp):
        gain_total = gain_total + sums[step]
    gain_out[...] = gain_total

    first = 1 if relayed else 0
    wait_bytes(chip_in.at[pl.ds(first, last - first)], chip_recv)
    for piece in range(pieces):
        result = chip_out[last, piece]
        for slot in range(first, last):
            result = result + chip_in[slot, piece]
        attn[:, piece * LANES : (piece + 1) * LANES] = result.astype(jnp.bfloat16)

    wait_bytes(stats.at[pl.ds(1, tp - 1)], send_sem.at[0])
    wait_bytes(pair_out, send_sem.at[1])
    wait_bytes(chip_in.at[pl.ds(first, last - first)], send_sem.at[3])
    if relayed:
        wait_bytes(early_out, send_sem.at[2])
        wait_bytes(relay_in.at[:, pl.ds(early, rows - early)], send_sem.at[4])
    wait_bytes(sums.at[pl.ds(1, dp - 1)], send_sem.at[5])


def write_results(resid, attn, gain, resid_out, attn_out, gain_out, sem):
    copies = [
        pltpu.make_async_copy(source, target, sem.at[i])
        for i, (source, target) in enumerate(
            ((resid, resid_out), (attn, attn_out), (gain, gain_out))
        )
    ]
    for copy in copies:
        copy.start()
    for copy in copies:
        copy.wait()


def on_device(tp, dp, features, grad_out, hidden_sum, norm_gain, out_weight):
    rows, width = grad_out.shape
    block = out_weight.shape[0] // tp
    half = tp // 2
    pieces = block // LANES
    parts = cuts(rows, half == 4 and pieces % 2 == 0)
    early = parts[0][1]
    anywhere = pl.BlockSpec(memory_space=pltpu.HBM)
    vmem = pl.BlockSpec(memory_space=pltpu.VMEM)
    dma = pltpu.SemaphoreType.DMA
    resid, attn, gain = pl.pallas_call(
        functools.partial(kernel, tp, dp, features),
        out_shape=(
            jax.ShapeDtypeStruct((rows, width), jnp.bfloat16),
            jax.ShapeDtypeStruct((rows, block), jnp.bfloat16),
            jax.ShapeDtypeStruct((1, width), jnp.float32),
        ),
        in_specs=[anywhere, anywhere, anywhere, anywhere],
        out_specs=(vmem, vmem, vmem),
        scratch_shapes=[
            pltpu.VMEM((rows, width), jnp.bfloat16),
            pltpu.VMEM((2 * rows, width), jnp.bfloat16),
            pltpu.VMEM((1, width), jnp.float32),
            pltpu.VMEM((half, 2 * block, width), jnp.bfloat16),
            pltpu.VMEM((tp, 2, rows), jnp.float32),
            pltpu.VMEM((half, 2, rows, block), jnp.float32),
            pltpu.VMEM((half, 2, rows, block), jnp.float32),
            pltpu.VMEM((half, 2, rows, block), jnp.float32),
            pltpu.VMEM((half, pieces, rows, LANES), jnp.float32),
            pltpu.VMEM((half, pieces, rows, LANES), jnp.float32),
            pltpu.VMEM((pieces, 2, early, LANES), jnp.float32),
            pltpu.VMEM((pieces, 2, early, LANES), jnp.float32),
            pltpu.VMEM((pieces, rows, LANES), jnp.float32),
            pltpu.VMEM((dp, 1, width), jnp.float32),
            dma((BANDS + 1,)),
            dma((half,)),
            dma((6,)),
            pltpu.SemaphoreType.DMA,
            dma((half,)),
            dma((pieces,)),
            dma((pieces, max(len(parts) - 1, 1))),
            pltpu.SemaphoreType.DMA,
            pltpu.SemaphoreType.DMA,
            pltpu.SemaphoreType.REGULAR,
        ],
        compiler_params=pltpu.CompilerParams(
            collective_id=0, has_side_effects=True, vmem_limit_bytes=52 * 2**20
        ),
        name="backward",
    )(
        pltpu.with_memory_space_constraint(grad_out, pltpu.HBM),
        pltpu.with_memory_space_constraint(hidden_sum, pltpu.HBM),
        pltpu.with_memory_space_constraint(norm_gain.reshape(1, width), pltpu.HBM),
        pltpu.with_memory_space_constraint(out_weight, pltpu.HBM),
    )
    resid, attn, gain = pl.pallas_call(
        write_results,
        out_shape=(
            jax.ShapeDtypeStruct((rows, width), jnp.bfloat16),
            jax.ShapeDtypeStruct((rows, block), jnp.bfloat16),
            jax.ShapeDtypeStruct((1, width), jnp.float32),
        ),
        in_specs=[vmem, vmem, vmem],
        out_specs=(anywhere, anywhere, anywhere),
        scratch_shapes=[dma((3,))],
        compiler_params=pltpu.CompilerParams(vmem_limit_bytes=4 * 2**20),
        name="write_results",
    )(resid, attn, gain)
    return resid, attn, gain.reshape(width)


def solution(mesh):
    tp, dp = mesh.shape["tp"], mesh.shape["dp"]

    def whole(grad_out, hidden_sum, norm_gain, out_weight):
        features = grad_out.shape[1]
        return jax.shard_map(
            functools.partial(on_device, tp, dp, features),
            mesh=mesh,
            in_specs=(P("dp", "tp"), P("dp", "tp"), P("tp"), P(None, "tp")),
            out_specs=(P("dp", "tp"), P("dp", "tp"), P("tp")),
            check_vma=False,
        )(grad_out, hidden_sum, norm_gain, out_weight)

    return whole
```

```python
import functools

import jax
import jax.numpy as jnp
from jax import lax
from jax.experimental import pallas as pl
from jax.experimental.pallas import tpu as pltpu
from jax.sharding import PartitionSpec as P

EPSILON = 1e-05
MESH = pl.DeviceIdType.MESH
LANES = 128
BANDS = 4


def flipped(index, mask):
    result, bit = index, 1
    while bit <= mask:
        if mask & bit:
            result = result + bit * (1 - 2 * lax.rem(lax.div(index, bit), 2))
        bit *= 2
    return result


def cuts(rows, relayed):
    if not relayed:
        return [(0, rows)]
    half, quarter = rows // 2, rows // 4
    return [(0, half), (half, quarter), (half + quarter, quarter)]


def kernel(
    tp, dp, features,
    grad_hbm, hidden_hbm, gain_hbm, weight_hbm,
    resid, attn, gain_out,
    grad, both, gain_ref, weight, stats, pair_out, pair_in, pair_own, chip_out, chip_in,
    early_out, early_in, relay_in, sums, crossed,
    load_sem, weight_sem, send_sem, stat_recv, pair_recv, early_recv, relay_recv, chip_recv,
    sum_recv, ready,
):
    me = lax.axis_index("tp")
    z = lax.axis_index("dp")
    core = lax.rem(me, 2)
    rows, width = grad.shape
    block = attn.shape[1]
    hidden = both.at[pl.ds(rows, rows), :]
    steps = width // LANES
    band = rows // BANDS
    pieces = block // LANES
    order = sorted(range(0, tp, 2), key=lambda mask: (-bin(mask).count("1"), mask))
    last = len(order) - 1
    relayed = len(order) == 4 and pieces % 2 == 0
    parts = cuts(rows, relayed)
    early = parts[0][1]

    def remote(source, target, kind, recv_sem, axis, index):
        return pltpu.make_async_remote_copy(
            src_ref=source,
            dst_ref=target,
            send_sem=send_sem.at[kind],
            recv_sem=recv_sem,
            device_id={axis: index},
            device_id_type=MESH,
        )

    def wait_bytes(ref, sem):
        pltpu.make_async_copy(ref, ref, sem).wait()

    load_gain = pltpu.make_async_copy(gain_hbm, gain_ref, load_sem.at[BANDS])
    for part in range(BANDS):
        at = pl.ds(part * band, band)
        pltpu.make_async_copy(
            hidden_hbm.at[at, :],
            both.at[pl.ds(rows + part * band, band), :],
            load_sem.at[part],
        ).start()
        pltpu.make_async_copy(grad_hbm.at[at, :], grad.at[at, :], load_sem.at[part]).start()
        if part == 0:
            load_gain.start()

    barrier = pltpu.get_barrier_semaphore()
    for mask in range(1, tp):
        pl.semaphore_signal(
            barrier, inc=1, device_id={"tp": flipped(me, mask)}, device_id_type=MESH
        )
    for step in range(1, dp):

        @pl.when(z + step < dp)
        def _():
            pl.semaphore_signal(
                barrier, inc=1, device_id={"dp": z + step}, device_id_type=MESH
            )

    weight_loads = []
    for slot, chip in enumerate(order):
        start = pl.multiple_of((flipped(me, chip) - core) * block, 2 * block)
        load = pltpu.make_async_copy(
            weight_hbm.at[pl.ds(start, 2 * block), :], weight.at[slot], weight_sem.at[slot]
        )
        load.start()
        weight_loads.append(load)

    load_gain.wait()
    squares, dotted = [], []
    for part in range(BANDS):
        wait_bytes(grad.at[pl.ds(0, 2 * band), :], load_sem.at[part])
        at_rows = slice(part * band, (part + 1) * band)
        band_squares = jnp.zeros((band, LANES), jnp.float32)
        band_dotted = jnp.zeros((band, LANES), jnp.float32)
        for k in range(steps):
            at = slice(k * LANES, (k + 1) * LANES)
            h = hidden[at_rows, at].astype(jnp.float32)
            g = grad[at_rows, at].astype(jnp.float32)
            band_squares += h * h
            band_dotted += gain_ref[:, at] * g * h
        squares.append(band_squares)
        dotted.append(band_dotted)
    squares = jnp.concatenate(squares, axis=0)
    dotted = jnp.concatenate(dotted, axis=0)
    local_factor = jnp.sum(dotted, axis=1, keepdims=True) / (
        jnp.sum(squares, axis=1, keepdims=True) + width * EPSILON
    )
    stats[0, 0:1, :] = jnp.sum(squares.T, axis=0, keepdims=True)
    stats[0, 1:2, :] = jnp.sum(dotted.T, axis=0, keepdims=True)

    pl.semaphore_wait(barrier, tp - 1 + z)
    for mask in sorted(range(1, tp), key=lambda mask: (-bin(mask).count("1"), mask)):
        remote(
            stats.at[0], stats.at[mask], 0, stat_recv, "tp", flipped(me, mask)
        ).start()
    for step in range(1, dp):

        @pl.when(z >= step)
        def _():
            pl.semaphore_signal(
                ready, inc=1, device_id={"dp": z - step}, device_id_type=MESH
            )

    for k in range(steps):
        at = slice(k * LANES, (k + 1) * LANES)
        h = hidden[:, at].astype(jnp.float32)
        g = grad[:, at].astype(jnp.float32)
        both[0:rows, at] = (gain_ref[:, at] * g - h * local_factor).astype(jnp.bfloat16)

    def products(slot, which, target):
        out = lax.dot_general(
            both[...],
            weight[slot, pl.ds(pl.multiple_of(which * block, block), block)],
            (((1,), (1,)), ((), ())),
            preferred_element_type=jnp.float32,
        )
        target[0] = out[0:rows] + local_factor * out[rows:]
        target[1] = out[rows:]

    pair_copies = []

    def pair_step(slot):
        weight_loads[slot].wait()
        copy = remote(
            pair_out.at[slot], pair_in.at[slot], 1, pair_recv.at[slot], "tp", flipped(me, 1)
        )
        products(slot, 1 - core, pair_out.at[slot])
        if slot < 0:
            copy.start()
        products(slot, core, pair_own.at[slot])
        if slot >= 0:
            copy.start()
        pair_copies.append(copy)

    for slot in range(min(last, 2)):
        pair_step(slot)

    def relay(piece, source, target, kind, recv_sem):
        copy = remote(
            source, target, kind, recv_sem, "tp", flipped(me, order[1 + piece % 2])
        )
        copy.start()
        return copy

    early_copies = []
    pair_copies[0].wait_recv()
    if relayed:
        for piece in range(pieces):
            at = slice(piece * LANES, (piece + 1) * LANES)
            for plane in range(2):
                early_out[piece, plane] = (
                    pair_own[0, plane, 0:early, at] + pair_in[0, plane, 0:early, at]
                )
            early_copies.append(
                relay(piece, early_out.at[piece], early_in.at[piece], 2, early_recv.at[piece])
            )

    for slot in range(2, last):
        pair_step(slot)

    for k in range(steps):
        at = slice(k * LANES, (k + 1) * LANES)
        crossed[:, at] = hidden[:, at].astype(jnp.float32) * grad[:, at].astype(jnp.float32)

    wait_bytes(stats.at[pl.ds(1, tp - 1)], stat_recv)
    total = stats[0]
    for mask in range(1, tp):
        total = total + stats[mask]
    inverse_row = lax.rsqrt(total[0:1, :] / features + EPSILON)
    factor_row = inverse_row * inverse_row * total[1:2, :] / features
    inverse = jnp.broadcast_to(inverse_row, (LANES, rows)).T
    factor = jnp.broadcast_to(factor_row, (LANES, rows)).T

    for k in range(steps):
        at = slice(k * LANES, (k + 1) * LANES)
        sums[0, :, at] = jnp.sum(crossed[:, at] * inverse, axis=0, keepdims=True)
    sum_copies = []
    for step in range(1, dp):
        copy = remote(
            sums.at[0], sums.at[step], 5, sum_recv, "dp", lax.rem(z + step, dp)
        )
        pl.when(z + step >= dp)(copy.start)
        sum_copies.append((step, copy))

    def chip_piece(slot, piece, low=0, high=rows):
        at = slice(piece * LANES, (piece + 1) * LANES)
        own, got = pair_own.at[slot, :, low:high, at], pair_in.at[slot, :, low:high, at]
        gained = own[0] + got[0]
        plain = own[1] + got[1]
        chip_out[slot, piece, low:high] = inverse[low:high] * (
            gained - factor[low:high] * plain
        )

    def send(slot, piece, part):
        at = pl.ds(*parts[part])
        remote(
            chip_out.at[slot, piece, at],
            chip_in.at[slot, piece, at],
            3,
            chip_recv,
            "tp",
            flipped(me, order[slot]),
        ).start()

    relay_copies = []
    if relayed:
        for part in range(1, len(parts)):
            low, size = parts[part]
            for piece in range(pieces):
                chip_piece(0, piece, low, low + size)
                relay_copies.append(
                    relay(
                        piece,
                        chip_out.at[0, piece, pl.ds(low, size)],
                        relay_in.at[piece, pl.ds(low, size)],
                        4,
                        relay_recv.at[piece, part - 1],
                    )
                )
    else:
        for piece in range(pieces):
            chip_piece(0, piece)
            send(0, piece, 0)
    for slot in range(1, last):
        pair_copies[slot].wait_recv()
        for piece in range(pieces):
            chip_piece(slot, piece)
            if not relayed or piece % 2 == slot - 1:
                for part in range(len(parts)):
                    send(slot, piece, part)

    pair_step(last)

    for k in range(steps):
        at = slice(k * LANES, (k + 1) * LANES)
        h = hidden[:, at].astype(jnp.float32)
        g = grad[:, at].astype(jnp.float32)
        value = inverse * (gain_ref[:, at] * g - h * factor)
        resid[:, at] = value.astype(jnp.bfloat16)

    @pl.when(z < dp - 1)
    def _():
        pl.semaphore_wait(ready, dp - 1 - z)

    for step, copy in reversed(sum_copies):
        pl.when(z + step < dp)(copy.start)

    if relayed:
        for piece in range(pieces):
            slot = 2 - piece % 2
            early_copies[piece].wait_recv()
            chip_out[slot, piece, 0:early] = chip_out[slot, piece, 0:early] + inverse[
                0:early
            ] * (early_in[piece, 0] - factor[0:early] * early_in[piece, 1])
            send(slot, piece, 0)
        for i, copy in enumerate(relay_copies):
            part, piece = 1 + i // pieces, i % pieces
            slot = 2 - piece % 2
            low, size = parts[part]
            at = slice(low, low + size)
            copy.wait_recv()
            chip_out[slot, piece, at] = chip_out[slot, piece, at] + relay_in[piece, at]
            send(slot, piece, part)

    pair_copies[last].wait_recv()
    for piece in range(pieces):
        chip_piece(last, piece)

    wait_bytes(sums.at[pl.ds(1, dp - 1)], sum_recv)
    gain_total = sums[0]
    for step in range(1, dp):
        gain_total = gain_total + sums[step]
    gain_out[...] = gain_total

    first = 1 if relayed else 0
    wait_bytes(chip_in.at[pl.ds(first, last - first)], chip_recv)
    for piece in range(pieces):
        result = chip_out[last, piece]
        for slot in range(first, last):
            result = result + chip_in[slot, piece]
        attn[:, piece * LANES : (piece + 1) * LANES] = result.astype(jnp.bfloat16)

    wait_bytes(stats.at[pl.ds(1, tp - 1)], send_sem.at[0])
    wait_bytes(pair_out, send_sem.at[1])
    wait_bytes(chip_in.at[pl.ds(first, last - first)], send_sem.at[3])
    if relayed:
        wait_bytes(early_out, send_sem.at[2])
        wait_bytes(relay_in.at[:, pl.ds(early, rows - early)], send_sem.at[4])
    wait_bytes(sums.at[pl.ds(1, dp - 1)], send_sem.at[5])


def write_results(resid, attn, gain, resid_out, attn_out, gain_out, sem):
    copies = [
        pltpu.make_async_copy(source, target, sem.at[i])
        for i, (source, target) in enumerate(
            ((resid, resid_out), (attn, attn_out), (gain, gain_out))
        )
    ]
    for copy in copies:
        copy.start()
    for copy in copies:
        copy.wait()


def on_device(tp, dp, features, grad_out, hidden_sum, norm_gain, out_weight):
    rows, width = grad_out.shape
    block = out_weight.shape[0] // tp
    half = tp // 2
    pieces = block // LANES
    parts = cuts(rows, half == 4 and pieces % 2 == 0)
    early = parts[0][1]
    anywhere = pl.BlockSpec(memory_space=pltpu.HBM)
    vmem = pl.BlockSpec(memory_space=pltpu.VMEM)
    dma = pltpu.SemaphoreType.DMA
    resid, attn, gain = pl.pallas_call(
        functools.partial(kernel, tp, dp, features),
        out_shape=(
            jax.ShapeDtypeStruct((rows, width), jnp.bfloat16),
            jax.ShapeDtypeStruct((rows, block), jnp.bfloat16),
            jax.ShapeDtypeStruct((1, width), jnp.float32),
        ),
        in_specs=[anywhere, anywhere, anywhere, anywhere],
        out_specs=(vmem, vmem, vmem),
        scratch_shapes=[
            pltpu.VMEM((rows, width), jnp.bfloat16),
            pltpu.VMEM((2 * rows, width), jnp.bfloat16),
            pltpu.VMEM((1, width), jnp.float32),
            pltpu.VMEM((half, 2 * block, width), jnp.bfloat16),
            pltpu.VMEM((tp, 2, rows), jnp.float32),
            pltpu.VMEM((half, 2, rows, block), jnp.float32),
            pltpu.VMEM((half, 2, rows, block), jnp.float32),
            pltpu.VMEM((half, 2, rows, block), jnp.float32),
            pltpu.VMEM((half, pieces, rows, LANES), jnp.float32),
            pltpu.VMEM((half, pieces, rows, LANES), jnp.float32),
            pltpu.VMEM((pieces, 2, early, LANES), jnp.float32),
            pltpu.VMEM((pieces, 2, early, LANES), jnp.float32),
            pltpu.VMEM((pieces, rows, LANES), jnp.float32),
            pltpu.VMEM((dp, 1, width), jnp.float32),
            pltpu.VMEM((rows, width), jnp.float32),
            dma((BANDS + 1,)),
            dma((half,)),
            dma((6,)),
            pltpu.SemaphoreType.DMA,
            dma((half,)),
            dma((pieces,)),
            dma((pieces, max(len(parts) - 1, 1))),
            pltpu.SemaphoreType.DMA,
            pltpu.SemaphoreType.DMA,
            pltpu.SemaphoreType.REGULAR,
        ],
        compiler_params=pltpu.CompilerParams(
            collective_id=0, has_side_effects=True, vmem_limit_bytes=52 * 2**20
        ),
        name="backward",
    )(
        pltpu.with_memory_space_constraint(grad_out, pltpu.HBM),
        pltpu.with_memory_space_constraint(hidden_sum, pltpu.HBM),
        pltpu.with_memory_space_constraint(norm_gain.reshape(1, width), pltpu.HBM),
        pltpu.with_memory_space_constraint(out_weight, pltpu.HBM),
    )
    resid, attn, gain = pl.pallas_call(
        write_results,
        out_shape=(
            jax.ShapeDtypeStruct((rows, width), jnp.bfloat16),
            jax.ShapeDtypeStruct((rows, block), jnp.bfloat16),
            jax.ShapeDtypeStruct((1, width), jnp.float32),
        ),
        in_specs=[vmem, vmem, vmem],
        out_specs=(anywhere, anywhere, anywhere),
        scratch_shapes=[dma((3,))],
        compiler_params=pltpu.CompilerParams(vmem_limit_bytes=4 * 2**20),
        name="write_results",
    )(resid, attn, gain)
    return resid, attn, gain.reshape(width)


def solution(mesh):
    tp, dp = mesh.shape["tp"], mesh.shape["dp"]

    def whole(grad_out, hidden_sum, norm_gain, out_weight):
        features = grad_out.shape[1]
        return jax.shard_map(
            functools.partial(on_device, tp, dp, features),
            mesh=mesh,
            in_specs=(P("dp", "tp"), P("dp", "tp"), P("tp"), P(None, "tp")),
            out_specs=(P("dp", "tp"), P("dp", "tp"), P("tp")),
            check_vma=False,
        )(grad_out, hidden_sum, norm_gain, out_weight)

    return whole
```

```python
import functools

import jax
import jax.numpy as jnp
from jax import lax
from jax.experimental import pallas as pl
from jax.experimental.pallas import tpu as pltpu
from jax.sharding import PartitionSpec as P

EPSILON = 1e-05
MESH = pl.DeviceIdType.MESH
LANES = 128
BANDS = 4
PARTS = 4
EARLY = 2
HALVES = 4


def flipped(index, mask):
    result, bit = index, 1
    while bit <= mask:
        if mask & bit:
            result = result + bit * (1 - 2 * lax.rem(lax.div(index, bit), 2))
        bit *= 2
    return result


def cuts(rows, number):
    part = rows // number
    return [(i * part, part) for i in range(number)]


def kernel(
    tp, dp, features,
    grad_hbm, hidden_hbm, gain_hbm, weight_hbm,
    resid, attn, gain_out,
    grad, both, gain_ref, weight, stats, pair_out, pair_in, pair_own, chip_out, chip_in,
    early_out, early_in, second_in, relay_in, handed, sums, crossed,
    load_sem, weight_sem, send_sem, stat_recv, pair_recv, first_recv, early_recv, relay_recv, handed_recv, chip_recv,
    sum_recv, ready,
):
    me = lax.axis_index("tp")
    z = lax.axis_index("dp")
    core = lax.rem(me, 2)
    rows, width = grad.shape
    block = attn.shape[1]
    hidden = both.at[pl.ds(rows, rows), :]
    steps = width // LANES
    band = rows // BANDS
    pieces = block // LANES
    order = sorted(range(0, tp, 2), key=lambda mask: (-bin(mask).count("1"), mask))
    last = len(order) - 1
    relayed = len(order) == 4 and pieces % 2 == 0
    parts, halves = cuts(rows, PARTS), cuts(rows, HALVES)

    def remote(source, target, kind, recv_sem, axis, index):
        return pltpu.make_async_remote_copy(
            src_ref=source,
            dst_ref=target,
            send_sem=send_sem.at[kind],
            recv_sem=recv_sem,
            device_id={axis: index},
            device_id_type=MESH,
        )

    def wait_bytes(ref, sem):
        pltpu.make_async_copy(ref, ref, sem).wait()

    load_gain = pltpu.make_async_copy(gain_hbm, gain_ref, load_sem.at[BANDS])
    for part in range(BANDS):
        at = pl.ds(part * band, band)
        pltpu.make_async_copy(
            hidden_hbm.at[at, :],
            both.at[pl.ds(rows + part * band, band), :],
            load_sem.at[part],
        ).start()
        pltpu.make_async_copy(grad_hbm.at[at, :], grad.at[at, :], load_sem.at[part]).start()
        if part == 0:
            load_gain.start()

    barrier = pltpu.get_barrier_semaphore()
    for mask in range(1, tp):
        pl.semaphore_signal(
            barrier, inc=1, device_id={"tp": flipped(me, mask)}, device_id_type=MESH
        )
    for step in range(1, dp):

        @pl.when(z + step < dp)
        def _():
            pl.semaphore_signal(
                barrier, inc=1, device_id={"dp": z + step}, device_id_type=MESH
            )

    weight_loads = []
    for slot, chip in enumerate(order):
        start = pl.multiple_of((flipped(me, chip) - core) * block, 2 * block)
        load = pltpu.make_async_copy(
            weight_hbm.at[pl.ds(start, 2 * block), :], weight.at[slot], weight_sem.at[slot]
        )
        load.start()
        weight_loads.append(load)

    load_gain.wait()
    squares, dotted = [], []
    for part in range(BANDS):
        wait_bytes(grad.at[pl.ds(0, 2 * band), :], load_sem.at[part])
        at_rows = slice(part * band, (part + 1) * band)
        band_squares = jnp.zeros((band, LANES), jnp.float32)
        band_dotted = jnp.zeros((band, LANES), jnp.float32)
        for k in range(steps):
            at = slice(k * LANES, (k + 1) * LANES)
            h = hidden[at_rows, at].astype(jnp.float32)
            g = grad[at_rows, at].astype(jnp.float32)
            band_squares += h * h
            band_dotted += gain_ref[:, at] * g * h
        squares.append(band_squares)
        dotted.append(band_dotted)
    squares = jnp.concatenate(squares, axis=0)
    dotted = jnp.concatenate(dotted, axis=0)
    local_factor = jnp.sum(dotted, axis=1, keepdims=True) / (
        jnp.sum(squares, axis=1, keepdims=True) + width * EPSILON
    )
    stats[0, 0:1, :] = jnp.sum(squares.T, axis=0, keepdims=True)
    stats[0, 1:2, :] = jnp.sum(dotted.T, axis=0, keepdims=True)

    pl.semaphore_wait(barrier, tp - 1 + z)
    for mask in sorted(range(1, tp), key=lambda mask: (-bin(mask).count("1"), mask)):
        remote(
            stats.at[0], stats.at[mask], 0, stat_recv, "tp", flipped(me, mask)
        ).start()
    for step in range(1, dp):

        @pl.when(z >= step)
        def _():
            pl.semaphore_signal(
                ready, inc=1, device_id={"dp": z - step}, device_id_type=MESH
            )

    for k in range(steps):
        at = slice(k * LANES, (k + 1) * LANES)
        h = hidden[:, at].astype(jnp.float32)
        g = grad[:, at].astype(jnp.float32)
        both[0:rows, at] = (gain_ref[:, at] * g - h * local_factor).astype(jnp.bfloat16)

    def products(slot, which, target):
        out = lax.dot_general(
            both[...],
            weight[slot, pl.ds(pl.multiple_of(which * block, block), block)],
            (((1,), (1,)), ((), ())),
            preferred_element_type=jnp.float32,
        )
        target[0] = out[0:rows] + local_factor * out[rows:]
        target[1] = out[rows:]

    pair_copies = []
    first_copies = [] if not relayed else [
        remote(
            pair_out.at[0, :, pl.ds(low, size)],
            pair_in.at[0, :, pl.ds(low, size)],
            1,
            first_recv.at[part],
            "tp",
            flipped(me, 1),
        )
        for part, (low, size) in enumerate(halves)
    ]

    def pair_step(slot):
        weight_loads[slot].wait()
        products(slot, 1 - core, pair_out.at[slot])
        products(slot, core, pair_own.at[slot])
        if slot == 0 and relayed:
            for copy in first_copies:
                copy.start()
            pair_copies.append(None)
        else:
            copy = remote(
                pair_out.at[slot],
                pair_in.at[slot],
                1,
                pair_recv.at[slot],
                "tp",
                flipped(me, 1),
            )
            copy.start()
            pair_copies.append(copy)

    for slot in range(min(last, 2)):
        pair_step(slot)

    def early_relay(piece, part):
        return remote(
            early_out.at[piece, part],
            early_in.at[piece, part],
            2,
            early_recv.at[piece, part],
            "tp",
            flipped(me, order[1 + piece % 2] + 1),
        )

    def late_relay(piece, half):
        at = pl.ds(*halves[half])
        return remote(
            chip_out.at[0, piece, at],
            relay_in.at[piece, at],
            2,
            relay_recv.at[piece, half],
            "tp",
            flipped(me, order[1 + piece % 2]),
        )

    def second_relay(piece, part):
        at = pl.ds(*parts[part])
        return remote(
            chip_out.at[0, piece, at],
            second_in.at[piece, at],
            6,
            early_recv.at[piece, part],
            "tp",
            flipped(me, order[1 + piece % 2] + 1),
        )

    early_relays = [(part, piece) for part in range(EARLY) for piece in range(pieces)]
    second_relays = [
        (part, piece) for part in range(EARLY, PARTS) for piece in range(pieces)
    ]
    late_relays = [(half, piece) for half in range(HALVES) for piece in range(pieces)]
    if not relayed:
        pair_copies[0].wait_recv()
    if relayed:

        @pl.when(core == 1)
        def _():
            for copy in first_copies:
                copy.wait_recv()

        @pl.when(core == 0)
        def _():
            for part, piece in early_relays:
                low, size = parts[part]
                if piece == 0 and part * HALVES % PARTS == 0:
                    first_copies[part * HALVES // PARTS].wait_recv()
                at = slice(piece * LANES, (piece + 1) * LANES)
                for plane in range(2):
                    early_out[piece, part, plane] = (
                        pair_own[0, plane, low : low + size, at]
                        + pair_in[0, plane, low : low + size, at]
                    )
                early_relay(piece, part).start()
            for half in range((EARLY - 1) * HALVES // PARTS + 1, HALVES):
                first_copies[half].wait_recv()

    for slot in range(2, last):
        pair_step(slot)

    for k in range(steps):
        at = slice(k * LANES, (k + 1) * LANES)
        crossed[:, at] = hidden[:, at].astype(jnp.float32) * grad[:, at].astype(jnp.float32)

    wait_bytes(stats.at[pl.ds(1, tp - 1)], stat_recv)
    total = stats[0]
    for mask in range(1, tp):
        total = total + stats[mask]
    inverse_row = lax.rsqrt(total[0:1, :] / features + EPSILON)
    factor_row = inverse_row * inverse_row * total[1:2, :] / features
    inverse = jnp.broadcast_to(inverse_row, (LANES, rows)).T
    factor = jnp.broadcast_to(factor_row, (LANES, rows)).T

    def chip_piece(slot, piece, low=0, high=rows):
        at = slice(piece * LANES, (piece + 1) * LANES)
        own, got = pair_own.at[slot, :, low:high, at], pair_in.at[slot, :, low:high, at]
        gained = own[0] + got[0]
        plain = own[1] + got[1]
        chip_out[slot, piece, low:high] = inverse[low:high] * (
            gained - factor[low:high] * plain
        )

    def send(slot, piece, low=0, size=rows):
        at = pl.ds(low, size)
        remote(
            chip_out.at[slot, piece, at],
            chip_in.at[slot, piece, at],
            3,
            chip_recv,
            "tp",
            flipped(me, order[slot]),
        ).start()

    if relayed:

        @pl.when(core == 0)
        def _():
            for part, piece in second_relays:
                low, size = parts[part]
                chip_piece(0, piece, low, low + size)
                second_relay(piece, part).start()

    if relayed:

        @pl.when(core == 1)
        def _():
            for half, piece in late_relays:
                low, size = halves[half]
                chip_piece(0, piece, low, low + size)
                late_relay(piece, half).start()

    else:
        for piece in range(pieces):
            chip_piece(0, piece)
            send(0, piece)
    for k in range(steps):
        at = slice(k * LANES, (k + 1) * LANES)
        sums[0, :, at] = jnp.sum(crossed[:, at] * inverse, axis=0, keepdims=True)
    sum_copies = []
    for step in range(1, dp):
        copy = remote(
            sums.at[0], sums.at[step], 4, sum_recv, "dp", lax.rem(z + step, dp)
        )
        pl.when(z + step >= dp)(copy.start)
        sum_copies.append((step, copy))

    def hand(slot, piece):
        return remote(
            chip_out.at[slot, piece], handed.at[piece], 5, handed_recv, "tp", flipped(me, 1)
        )

    for slot in range(1, last):
        pair_copies[slot].wait_recv()
        for piece in range(pieces):
            chip_piece(slot, piece)
            if not relayed or piece % 2 == slot - 1:
                send(slot, piece)
            else:
                pl.when(core == 0)(hand(slot, piece).start)

    pair_step(last)

    for k in range(steps):
        at = slice(k * LANES, (k + 1) * LANES)
        h = hidden[:, at].astype(jnp.float32)
        g = grad[:, at].astype(jnp.float32)
        value = inverse * (gain_ref[:, at] * g - h * factor)
        resid[:, at] = value.astype(jnp.bfloat16)

    if relayed:

        @pl.when(core == 1)
        def _():
            wait_bytes(handed, handed_recv)
            for part, piece in early_relays + second_relays:
                low, size = parts[part]
                slot, at = 2 - piece % 2, slice(low, low + size)
                if part < EARLY:
                    early_relay(piece, part).wait_recv()
                    got = inverse[at] * (
                        early_in[piece, part, 0] - factor[at] * early_in[piece, part, 1]
                    )
                else:
                    second_relay(piece, part).wait_recv()
                    got = second_in[piece, at]
                handed[piece, at] = handed[piece, at] + got
                remote(
                    handed.at[piece, pl.ds(low, size)],
                    chip_in.at[slot, piece, pl.ds(low, size)],
                    5,
                    chip_recv,
                    "tp",
                    flipped(me, order[slot] + 1),
                ).start()
            for half, piece in late_relays:
                low, size = halves[half]
                slot, at = 2 - piece % 2, slice(low, low + size)
                late_relay(piece, half).wait_recv()
                chip_out[slot, piece, at] = chip_out[slot, piece, at] + relay_in[piece, at]
                send(slot, piece, low, size)

    @pl.when(z < dp - 1)
    def _():
        pl.semaphore_wait(ready, dp - 1 - z)

    for step, copy in reversed(sum_copies):
        pl.when(z + step < dp)(copy.start)

    pair_copies[last].wait_recv()
    for piece in range(pieces):
        chip_piece(last, piece)

    wait_bytes(sums.at[pl.ds(1, dp - 1)], sum_recv)
    gain_total = sums[0]
    for step in range(1, dp):
        gain_total = gain_total + sums[step]
    gain_out[...] = gain_total

    first = 1 if relayed else 0
    wait_bytes(chip_in.at[pl.ds(first, last - first)], chip_recv)
    for piece in range(pieces):
        result = chip_out[last, piece]
        for slot in range(first, last):
            result = result + chip_in[slot, piece]
        attn[:, piece * LANES : (piece + 1) * LANES] = result.astype(jnp.bfloat16)

    wait_bytes(stats.at[pl.ds(1, tp - 1)], send_sem.at[0])
    wait_bytes(pair_out, send_sem.at[1])
    wait_bytes(sums.at[pl.ds(1, dp - 1)], send_sem.at[4])
    if relayed:
        wait_bytes(handed, send_sem.at[5])

        @pl.when(core == 0)
        def _():
            wait_bytes(chip_in.at[1], send_sem.at[3])
            wait_bytes(early_out, send_sem.at[2])
            wait_bytes(second_in.at[:, pl.ds(parts[EARLY][0], rows - parts[EARLY][0])], send_sem.at[6])

        @pl.when(core == 1)
        def _():
            wait_bytes(chip_in.at[pl.ds(1, 2)], send_sem.at[3])
            wait_bytes(relay_in, send_sem.at[2])

    else:
        wait_bytes(chip_in.at[pl.ds(0, last)], send_sem.at[3])


def write_results(resid, attn, gain, resid_out, attn_out, gain_out, sem):
    copies = [
        pltpu.make_async_copy(source, target, sem.at[i])
        for i, (source, target) in enumerate(
            ((resid, resid_out), (attn, attn_out), (gain, gain_out))
        )
    ]
    for copy in copies:
        copy.start()
    for copy in copies:
        copy.wait()


def on_device(tp, dp, features, grad_out, hidden_sum, norm_gain, out_weight):
    rows, width = grad_out.shape
    block = out_weight.shape[0] // tp
    half = tp // 2
    pieces = block // LANES
    anywhere = pl.BlockSpec(memory_space=pltpu.HBM)
    vmem = pl.BlockSpec(memory_space=pltpu.VMEM)
    dma = pltpu.SemaphoreType.DMA
    resid, attn, gain = pl.pallas_call(
        functools.partial(kernel, tp, dp, features),
        out_shape=(
            jax.ShapeDtypeStruct((rows, width), jnp.bfloat16),
            jax.ShapeDtypeStruct((rows, block), jnp.bfloat16),
            jax.ShapeDtypeStruct((1, width), jnp.float32),
        ),
        in_specs=[anywhere, anywhere, anywhere, anywhere],
        out_specs=(vmem, vmem, vmem),
        scratch_shapes=[
            pltpu.VMEM((rows, width), jnp.bfloat16),
            pltpu.VMEM((2 * rows, width), jnp.bfloat16),
            pltpu.VMEM((1, width), jnp.float32),
            pltpu.VMEM((half, 2 * block, width), jnp.bfloat16),
            pltpu.VMEM((tp, 2, rows), jnp.float32),
            pltpu.VMEM((half, 2, rows, block), jnp.float32),
            pltpu.VMEM((half, 2, rows, block), jnp.float32),
            pltpu.VMEM((half, 2, rows, block), jnp.float32),
            pltpu.VMEM((half, pieces, rows, LANES), jnp.float32),
            pltpu.VMEM((half, pieces, rows, LANES), jnp.float32),
            pltpu.VMEM((pieces, EARLY, 2, rows // PARTS, LANES), jnp.float32),
            pltpu.VMEM((pieces, EARLY, 2, rows // PARTS, LANES), jnp.float32),
            pltpu.VMEM((pieces, rows, LANES), jnp.float32),
            pltpu.VMEM((pieces, rows, LANES), jnp.float32),
            pltpu.VMEM((pieces, rows, LANES), jnp.float32),
            pltpu.VMEM((dp, 1, width), jnp.float32),
            pltpu.VMEM((rows, width), jnp.float32),
            dma((BANDS + 1,)),
            dma((half,)),
            dma((7,)),
            pltpu.SemaphoreType.DMA,
            dma((half,)),
            dma((HALVES,)),
            dma((pieces, PARTS)),
            dma((pieces, HALVES)),
            pltpu.SemaphoreType.DMA,
            pltpu.SemaphoreType.DMA,
            pltpu.SemaphoreType.DMA,
            pltpu.SemaphoreType.REGULAR,
        ],
        compiler_params=pltpu.CompilerParams(
            collective_id=0, has_side_effects=True, vmem_limit_bytes=52 * 2**20
        ),
        name="backward",
    )(
        pltpu.with_memory_space_constraint(grad_out, pltpu.HBM),
        pltpu.with_memory_space_constraint(hidden_sum, pltpu.HBM),
        pltpu.with_memory_space_constraint(norm_gain.reshape(1, width), pltpu.HBM),
        pltpu.with_memory_space_constraint(out_weight, pltpu.HBM),
    )
    resid, attn, gain = pl.pallas_call(
        write_results,
        out_shape=(
            jax.ShapeDtypeStruct((rows, width), jnp.bfloat16),
            jax.ShapeDtypeStruct((rows, block), jnp.bfloat16),
            jax.ShapeDtypeStruct((1, width), jnp.float32),
        ),
        in_specs=[vmem, vmem, vmem],
        out_specs=(anywhere, anywhere, anywhere),
        scratch_shapes=[dma((3,))],
        compiler_params=pltpu.CompilerParams(vmem_limit_bytes=4 * 2**20),
        name="write_results",
    )(resid, attn, gain)
    return resid, attn, gain.reshape(width)


def solution(mesh):
    tp, dp = mesh.shape["tp"], mesh.shape["dp"]

    def whole(grad_out, hidden_sum, norm_gain, out_weight):
        features = grad_out.shape[1]
        return jax.shard_map(
            functools.partial(on_device, tp, dp, features),
            mesh=mesh,
            in_specs=(P("dp", "tp"), P("dp", "tp"), P("tp"), P(None, "tp")),
            out_specs=(P("dp", "tp"), P("dp", "tp"), P("tp")),
            check_vma=False,
        )(grad_out, hidden_sum, norm_gain, out_weight)

    return whole
```
